256 devices in a mesh: shard: 16 (over z, core), width: 4 (over x), shift: 4 (over y).
Axes of the slice: x: 4, y: 4, z: 8, core: 2. Of those that a mesh axis runs over, the one named last changes fastest.
Arguments:
- w_query: float32 [16384, 4096], P(('shift', 'shard'), 'width'), parts along dimension 0, may hold values from -0.125 to 0.125
- first_query: float32 [16384, 4096], P(('shift', 'shard'), 'width'), parts along dimension 0, may hold values from -0.09375 to 0.09375
- second_query: float32 [16384, 4096], P(('shift', 'shard'), 'width'), parts along dimension 0, may hold values from -0.09375 to 0.09375
- w_key: float32 [16384, 1024], P(('shift', 'shard'), 'width'), parts along dimension 0, may hold values from -0.125 to 0.125
- first_key: float32 [16384, 1024], P(('shift', 'shard'), 'width'), parts along dimension 0, may hold values from -0.09375 to 0.09375
- second_key: float32 [16384, 1024], P(('shift', 'shard'), 'width'), parts along dimension 0, may hold values from -0.09375 to 0.09375
- w_value: float32 [16384, 1024], P(('shift', 'shard'), 'width'), parts along dimension 0, may hold values from -0.125 to 0.125
- first_value: float32 [16384, 1024], P(('shift', 'shard'), 'width'), parts along dimension 0, may hold values from -0.09375 to 0.09375
- second_value: float32 [16384, 1024], P(('shift', 'shard'), 'width'), parts along dimension 0, may hold values from -0.09375 to 0.09375
- norm_gain: float32 [16384], P(('shift', 'shard')), parts along dimension 0, may hold values from 0.25 to 1.75
Outputs:
- ready_query: bfloat16 [16384, 4096], P('shift', 'width'), parts along dimension 0
- ready_key: bfloat16 [16384, 1024], P('shift', 'width'), parts along dimension 0
- ready_value: bfloat16 [16384, 1024], P('shift', 'width'), parts along dimension 0
- scale_query: float32 [16384], P(('shift', 'width')), parts along dimension 0
- scale_key: float32 [4096], P(('shift', 'width')), parts along dimension 0
- scale_value: float32 [4096], P(('shift', 'width')), parts along dimension 0
The draws below stay inside these ranges and needn't reach their ends.
There are 4 independent parts, one for each index of `shift`. The reference program is written for one: setup_inputs(seed, part) draws one part's arguments, and reference() takes and returns one part's arrays. A program takes and returns all parts, laid end to end along the dimension named above; each array names one. Nothing has to cross between parts.
All inputs are finite; a program needn't handle non-finite values. Where the reference program divides by a largest or mean magnitude, that divisor is 1e-20 or more.
Results may differ from the reference program's by a relative error of at most 0.001.
Values may be sent and summed in bfloat16 or wider, within the bound.
No kernel may reach another device: no remote copies, remote signals or barrier semaphores. Data moves between devices by JAX's collectives and lax.ppermute only.
A program may use at most 128 MiB of HBM per device.

```python
import jax
import jax.numpy as jnp

D_MODEL = 4096
Q_DIM = 4096
KV_DIM = 1024


def spiked(drawn, own_key, source, target, blocks, factor):
    owner, partner = [(jnp.arange(drawn.shape[axis_at]) // (drawn.shape[axis_at] // blocks)).reshape([-1 if axis == axis_at else 1 for axis in range(drawn.ndim)]) for axis_at in (source, target)]
    chosen = jax.random.permutation(own_key, blocks)[partner]
    strong = (owner == chosen) | (owner == (partner + blocks // 2) % blocks)
    return jnp.where(strong, factor * drawn, drawn)


def levels(rng, extent, shards, least, high):
    loudness, own = 1.0, jax.random.fold_in(rng, 6)
    for dim, blocks in shards:
        heights = jnp.exp(jax.random.uniform(jax.random.fold_in(own, dim), (blocks,), jnp.float32, least / len(shards), high / len(shards)))
        loudness = loudness * jnp.repeat(heights, extent[dim] // blocks).reshape([-1 if axis == dim else 1 for axis in range(len(extent))])
    return loudness


def noise(own_key, dims, deviation, limit, split=(), kind=jnp.bfloat16):
    array = deviation * jax.random.normal(own_key, dims, jnp.float32)
    if split:
        array = array * levels(own_key, dims, split, -0.22, 0.18)
    return jnp.clip(array, -limit, limit).astype(kind)


def bell_draw_with(own_key, extent, spread, limit, cuts, heavy, held_as=jnp.bfloat16):
    array = spread * jax.random.normal(own_key, extent, jnp.float32)
    if cuts:
        array = array * levels(own_key, extent, cuts, -0.22, 0.18)
    return jnp.clip(spiked(array, jax.random.fold_in(own_key, 3), *heavy), -limit, limit).astype(held_as)


def setup_inputs(seed: int = 0, part: int = 0) -> dict:
    arg_keys = jax.random.split(jax.random.key(seed), 11)
    part_splits = jax.random.split(jax.random.fold_in(arg_keys[10], part), 11)
    w_query = bell_draw_with(part_splits[0], (D_MODEL, Q_DIM), D_MODEL ** -0.5, 0.125, ((0, 16), (1, 4)), (0, 1, 16, 2.0), jnp.float32)
    first_query = noise(part_splits[1], (D_MODEL, Q_DIM), D_MODEL ** -0.5, 0.09375, ((0, 16), (1, 4)), jnp.float32)
    second_query = noise(part_splits[2], (D_MODEL, Q_DIM), D_MODEL ** -0.5, 0.09375, ((0, 16), (1, 4)), jnp.float32)
    w_key = bell_draw_with(part_splits[3], (D_MODEL, KV_DIM), D_MODEL ** -0.5, 0.125, ((0, 16), (1, 4)), (0, 1, 16, 2.0), jnp.float32)
    first_key = noise(part_splits[4], (D_MODEL, KV_DIM), D_MODEL ** -0.5, 0.09375, ((0, 16), (1, 4)), jnp.float32)
    second_key = noise(part_splits[5], (D_MODEL, KV_DIM), D_MODEL ** -0.5, 0.09375, ((0, 16), (1, 4)), jnp.float32)
    w_value = bell_draw_with(part_splits[6], (D_MODEL, KV_DIM), D_MODEL ** -0.5, 0.125, ((0, 16), (1, 4)), (0, 1, 16, 2.0), jnp.float32)
    first_value = noise(part_splits[7], (D_MODEL, KV_DIM), D_MODEL ** -0.5, 0.09375, ((0, 16), (1, 4)), jnp.float32)
    second_value = noise(part_splits[8], (D_MODEL, KV_DIM), D_MODEL ** -0.5, 0.09375, ((0, 16), (1, 4)), jnp.float32)
    norm_gain = jnp.clip(1.0 + 0.15 * jax.random.normal(part_splits[9], (D_MODEL,), jnp.float32), 0.25, 1.75)
    return dict(w_query=w_query, first_query=first_query, second_query=second_query, w_key=w_key, first_key=first_key, second_key=second_key, w_value=w_value, first_value=first_value, second_value=second_value, norm_gain=norm_gain)


learn_rate = 0.25
hold_rate = 0.8


def reference(w_query, first_query, second_query, w_key, first_key, second_key, w_value, first_value, second_value, norm_gain):
    hold_query = hold_rate * first_query + second_query
    latest_query = w_query - learn_rate * hold_query
    hold_key = hold_rate * first_key + second_key
    latest_key = w_key - learn_rate * hold_key
    hold_value = hold_rate * first_value + second_value
    latest_value = w_value - learn_rate * hold_value
    latest_gained_query = latest_query * norm_gain[:, None]
    latest_gained_key = latest_key * norm_gain[:, None]
    latest_gained_value = latest_value * norm_gain[:, None]
    scale_query = jnp.max(jnp.abs(latest_gained_query), axis=0)
    ready_query = (latest_gained_query / scale_query).astype(jnp.bfloat16)
    scale_key = jnp.max(jnp.abs(latest_gained_key), axis=0)
    ready_key = (latest_gained_key / scale_key).astype(jnp.bfloat16)
    scale_value = jnp.max(jnp.abs(latest_gained_value), axis=0)
    ready_value = (latest_gained_value / scale_value).astype(jnp.bfloat16)
    return ready_query, ready_key, ready_value, scale_query, scale_key, scale_value
```

```python
import functools

import jax
import jax.numpy as jnp
from jax import lax
from jax.experimental import pallas as pl
from jax.experimental.pallas import tpu as pltpu
from jax.sharding import PartitionSpec as P

learn_rate = 0.25
hold_rate = 0.8

N = 16
SWAP = [(i, i ^ 1) for i in range(N)]
RING = [(i, (i + 2) % N if i % 2 == 0 else (i - 2) % N) for i in range(N)]
WIDTHS = (1024, 256, 256)


def swap(x):
    return lax.ppermute(x, "shard", SWAP)


def shift(x):
    return lax.ppermute(x, "shard", RING)


def global_max(line):
    everyone = lax.all_to_all(jnp.broadcast_to(line[None], (N, *line.shape)), "shard", 0, 0, tiled=True)
    return jnp.max(everyone, axis=0)


def place_kernel(slots, count, *refs):
    rows, blocks = refs[0], refs[1 : 1 + count]
    outs, sem = refs[-4:-1], refs[-1]
    copies = []
    for b, (slot, block) in enumerate(zip(slots, blocks)):
        row = pl.multiple_of(rows[slot], 256)
        at = 0
        for o, (out, width) in enumerate(zip(outs, WIDTHS)):
            copies.append(
                pltpu.make_async_copy(
                    block.at[:, pl.ds(at, width)], out.at[pl.ds(row, 256), :], sem.at[b * 3 + o]
                )
            )
            at += width
    for c in copies:
        c.start()
    for c in copies:
        c.wait()


def place(rows, slots, blocks, outs):
    count = len(blocks)
    hbm = pl.BlockSpec(memory_space=pltpu.HBM)
    return pl.pallas_call(
        functools.partial(place_kernel, slots, count),
        out_shape=[jax.ShapeDtypeStruct((4096, w), jnp.bfloat16) for w in WIDTHS],
        in_specs=[pl.BlockSpec(memory_space=pltpu.SMEM)]
        + [pl.BlockSpec(memory_space=pl.ANY)] * count
        + [hbm] * (3 if outs else 0),
        out_specs=[hbm] * 3,
        scratch_shapes=[pltpu.SemaphoreType.DMA((3 * count,))],
        input_output_aliases={1 + count + i: i for i in range(3)} if outs else {},
        compiler_params=pltpu.CompilerParams(vmem_limit_bytes=1 << 20),
        cost_estimate=pl.CostEstimate(flops=1000000, bytes_accessed=2 * count * 786432, transcendentals=0),
        name="place",
    )(rows, *blocks, *(outs or ()))


def body(wq, fq, sq, wk, fk, sk, wv, fv, sv, gain):
    def gained(w, f, s):
        return (w - learn_rate * (hold_rate * f + s)) * gain[:, None]

    gq, gk, gv = gained(wq, fq, sq), gained(wk, fk, sk), gained(wv, fv, sv)
    line = jnp.concatenate([jnp.max(jnp.abs(g), axis=0) for g in (gq, gk, gv)])
    scale = global_max(line)
    s_q, s_k, s_v = scale[:1024], scale[1024:1280], scale[1280:]
    own = jnp.concatenate(
        [(gq / s_q).astype(jnp.bfloat16), (gk / s_k).astype(jnp.bfloat16), (gv / s_v).astype(jnp.bfloat16)], axis=1
    )
    me = lax.axis_index("shard")
    core = me & 1
    step = jnp.arange(8, dtype=jnp.int32)
    dist = 2 * ((step + 1) // 2)
    up = 1 - 2 * core
    same = jnp.where(step % 2 == 1, core, 1 - core)
    chip = me - core
    mine = ((chip - up * dist + 16) & 15) + same
    theirs = ((chip + up * dist + 16) & 15) + (1 - same)
    first = jnp.where(step == 0, me, mine)
    second = jnp.where(step == 0, me ^ 1, theirs)
    rows = 256 * jnp.concatenate([first, second])

    ring = [own]
    other = [swap(own)]
    ring.append(shift(own))
    ring.append(shift(other[0]))
    outs = place(rows, [0], [own], None)
    ring[1], *outs = lax.optimization_barrier((ring[1], *outs))
    for j in range(1, 8):
        if j <= 5:
            ring.append(shift(ring[j]))
        other.append(swap(ring[j]))
        outs = place(rows, [j, 8 + j - 1], [ring[j], other[j - 1]], outs)
        if j < 7:
            ring[j + 1], *outs = lax.optimization_barrier((ring[j + 1], *outs))
    outs = place(rows, [15], [other[7]], outs)
    return (*outs, s_q, s_k, s_v)


def solution(mesh):
    rows = P(("shift", "shard"), "width")
    cols = P(("shift", "width"))
    return jax.shard_map(
        body,
        mesh=mesh,
        in_specs=(rows,) * 9 + (P(("shift", "shard")),),
        out_specs=(P("shift", "width"),) * 3 + (cols,) * 3,
        check_vma=False,
    )
```
